32 devices in a mesh: dp: 8 (over z, y), col: 4 (over x, core).
Axes of the slice: x: 2, y: 2, z: 4, core: 2. Of those that a mesh axis runs over, the one named last changes fastest.
Arguments:
- view_first: bfloat16 [8192, 4096], P('dp'), may hold values from -1000 to 1000
- view_second: bfloat16 [8192, 4096], P('dp', 'col'), may hold values from -1000 to 1000
- valid_rows: int32 [8], P('dp'), may hold values from 1 to 1024, as said below
Outputs:
- correlation: float32 [4096, 4096], P('dp', 'col')
- loss: float32 [], replicated
The draws below stay inside these ranges and needn't reach their ends.
Inputs may be any that keep to these rules, and one draw needn't show every extreme that they name: `valid_rows`: some micro-batch uses all 1024 rows.
All inputs are finite; a program needn't handle non-finite values.
Results may differ from the reference program's by a relative error of at most 0.0005.
Values sent between devices are 32-bit elements; how exact they have to be, the bound alone decides.
A program may use at most 128 MiB of HBM per device.

```python
import math
import jax
import jax.numpy as jnp
from jax import lax

D = 4096
TOK_DEV = 1024
GROUPS = 8
TOKENS = 8192


def paired_views(key):
    keys = jax.random.split(jax.random.fold_in(key, 11), 9)
    steps = jnp.arange(GROUPS, dtype=jnp.float32)
    rising = 1.0 + 2.0 * steps / max(GROUPS - 1, 1)
    shift_first = jnp.clip(jax.random.normal(keys[0], (GROUPS, D)), -6.0, 6.0) * 1.5 * rising[:, None]
    other_shift = jnp.clip(jax.random.normal(keys[1], (GROUPS, D)), -6.0, 6.0) * 1.5 * rising[:, None]
    shift_second = 0.7 * shift_first + 0.7 * other_shift
    scale_first = jnp.exp(jax.random.uniform(keys[2], (D,), minval=0.0, maxval=math.log(10.0)))
    scale_second = jnp.exp(jax.random.uniform(keys[3], (D,), minval=0.0, maxval=math.log(10.0)))
    base = jnp.clip(jax.random.normal(keys[5], (TOKENS, D)), -6.0, 6.0)
    noise = jnp.clip(jax.random.normal(keys[6], (TOKENS, D)), -6.0, 6.0)
    center_first = jnp.clip(jax.random.normal(keys[7], (D,)), -6.0, 6.0)
    center_second = jnp.clip(jax.random.normal(keys[8], (D,)), -6.0, 6.0)
    rows_first = jnp.repeat(shift_first, TOK_DEV, axis=0)
    rows_second = jnp.repeat(shift_second, TOK_DEV, axis=0)
    first = (base + rows_first + center_first[None, :]) * scale_first[None, :]
    second = (0.8 * base + 0.6 * noise + rows_second + center_second[None, :]) * scale_second[None, :]
    return (first, second)


def draw_view_first(key, part):
    return paired_views(key)[0].astype(jnp.bfloat16)


def draw_view_second(key, part):
    return paired_views(key)[1].astype(jnp.bfloat16)


def draw_valid_rows(key, part):
    steps = jnp.arange(GROUPS, dtype=jnp.int32)
    lowest = TOK_DEV // 3
    rising = lowest + (TOK_DEV - lowest) * steps // max(GROUPS - 1, 1)
    jitter = jax.random.randint(jax.random.fold_in(key, 5), (GROUPS,), -(TOK_DEV // 8), 1)
    counts = jnp.clip(rising + jitter, 1, TOK_DEV)
    full_group = jax.random.randint(jax.random.fold_in(key, 9), (), 0, GROUPS)
    return jnp.where(steps == full_group, TOK_DEV, counts).astype(jnp.int32)


def setup_inputs(seed: int = 0) -> dict:
    key_list = jax.random.split(jax.random.key(seed), 4)
    return {
        "view_first": draw_view_first(jax.random.fold_in(key_list[3], 71), 0),
        "view_second": draw_view_second(jax.random.fold_in(key_list[3], 71), 0),
        "valid_rows": draw_valid_rows(jax.random.fold_in(key_list[3], 71), 0),
    }


epsilon = 1e-05
off_weight = 0.0051

def centered_group(block, used_rows):
    positions = jnp.arange(TOK_DEV, dtype=jnp.int32)
    live_col = (positions < used_rows)[:, None].astype(jnp.float32)
    used_float = used_rows.astype(jnp.float32)
    totals = lax.optimization_barrier(jnp.sum(block.astype(jnp.float32) * live_col, axis=0))
    means = totals / used_float
    centered = ((block.astype(jnp.float32) - means) * live_col).astype(jnp.bfloat16)
    return (totals, means, centered)

def reference(view_first, view_second, valid_rows):
    first = view_first.reshape(GROUPS, TOK_DEV, D)
    second = view_second.reshape(GROUPS, TOK_DEV, D)

    def group_terms(inputs):
        block_first, block_second, used_rows = inputs
        sum_first, mean_first, cent_first = centered_group(block_first, used_rows)
        sum_second, mean_second, cent_second = centered_group(block_second, used_rows)
        square_first = lax.optimization_barrier(jnp.sum(jnp.square(cent_first.astype(jnp.float32)), axis=0))
        square_second = lax.optimization_barrier(jnp.sum(jnp.square(cent_second.astype(jnp.float32)), axis=0))
        return (sum_first, sum_second, mean_first, mean_second, square_first, square_second)
    sums_first, sums_second, means_first, means_second, squares_first, squares_second = lax.map(group_terms, (first, second, valid_rows))
    counts = valid_rows.astype(jnp.float32)
    all_rows = jnp.sum(counts)
    glob_first = lax.optimization_barrier(jnp.sum(sums_first, axis=0)) / all_rows
    glob_second = lax.optimization_barrier(jnp.sum(sums_second, axis=0)) / all_rows
    shifts_first = means_first - glob_first[None, :]
    shifts_second = means_second - glob_second[None, :]
    spread_first = lax.optimization_barrier(jnp.sum(squares_first + counts[:, None] * jnp.square(shifts_first), axis=0))
    spread_second = lax.optimization_barrier(jnp.sum(squares_second + counts[:, None] * jnp.square(shifts_second), axis=0))

    def accumulate(running, inputs):
        block_first, block_second, used_rows, shift_first, shift_second = inputs
        cent_first = centered_group(block_first, used_rows)[2]
        cent_second = centered_group(block_second, used_rows)[2]
        product = jnp.dot(cent_first.T, cent_second, preferred_element_type=jnp.float32)
        used_float = used_rows.astype(jnp.float32)
        return (running + product + used_float * shift_first[:, None] * shift_second[None, :], None)
    moment, unused = lax.scan(accumulate, jnp.zeros((D, D), jnp.float32), (first, second, valid_rows, shifts_first, shifts_second))
    scale_first = jnp.sqrt(spread_first / all_rows + epsilon)
    scale_second = jnp.sqrt(spread_second / all_rows + epsilon)
    correlation = moment / (all_rows * scale_first[:, None] * scale_second[None, :])
    index_rows = jnp.arange(D, dtype=jnp.int32)
    diagonal = index_rows[:, None] == index_rows[None, :]
    terms = jnp.where(diagonal, jnp.square(1.0 - correlation), off_weight * jnp.square(correlation))
    loss = jnp.sum(terms) / D
    return (correlation, loss)
```

```python
import functools
import jax
import jax.numpy as jnp
from jax import lax
from jax.experimental import pallas as pl
from jax.experimental.pallas import tpu as pltpu
from jax.sharding import PartitionSpec as P

epsilon = 1e-05
off_weight = 0.0051
MESH = pl.DeviceIdType.MESH


def owner_at(place, length, step):
    low = jnp.minimum(place, length - 1 - place)
    high = length - 1 - low
    single = high - low
    rest = step - single
    upward = jnp.where(step < single, place == low, rest % 2 == 0)
    reach = jnp.where(step < single, high - step, low - rest // 2)
    return jnp.where(upward, place + reach, place - reach)


def reduce_kernel(
    n, x_ref, y_ref, st_ref, out_ref, stats_ref,
    pair_out, own, pair_in, line_in, own_b, line_in_b, swap_in, st_in,
    pair_ss, pair_rs, line_ss, line_rs, lineb_ss, lineb_rs, swap_ss, swap_rs, st_ss, st_rs,
):
    me = lax.axis_index("dp")
    length = n // 2
    place, side = me // 2, me % 2
    twin = place * 2 + (1 - side)
    rows = x_ref.shape[1]
    wide = own.shape[2]
    total = y_ref.shape[1]

    barrier = pltpu.get_barrier_semaphore()

    def greet(k, carry):
        pl.semaphore_signal(barrier, inc=1, device_id={"dp": (me + k) % n}, device_id_type=MESH)
        return carry

    lax.fori_loop(1, n, greet, 0)
    pl.semaphore_wait(barrier, n - 1)

    def remote(src, dst, ss, rs, target):
        return pltpu.make_async_remote_copy(
            src_ref=src, dst_ref=dst, send_sem=ss, recv_sem=rs,
            device_id={"dp": target}, device_id_type=MESH,
        )

    def stat_copy(k):
        peer = (me + k) % n
        return remote(st_ref.at[peer], st_in.at[k], st_ss.at[k], st_rs.at[k], peer)

    def pair_copy(j):
        return remote(pair_out.at[j], pair_in.at[j], pair_ss.at[j], pair_rs.at[j], twin)

    def ahead(owner):
        up = owner > place
        nearer = jnp.where(up, place + 1, place - 1)
        slot = jnp.where(jnp.logical_and(owner == nearer, jnp.logical_not(up)), length, owner)
        return nearer * 2 + side, slot

    def line_copy(owner, target, slot):
        return remote(own.at[owner], line_in.at[slot], line_ss.at[owner], line_rs.at[slot], target)

    def lineb_copy(owner, target, slot):
        return remote(own_b.at[owner], line_in_b.at[slot], lineb_ss.at[owner], lineb_rs.at[slot], target)

    def swap_copy():
        return remote(
            own_b.at[place, pl.ds((1 - side) * rows, rows)], swap_in, swap_ss.at[0], swap_rs.at[0], twin
        )

    def flow(owner, copy, buffer, landed):
        up = owner > place
        mine = owner == place
        from_low = jnp.logical_and(jnp.logical_or(up, mine), place > 0)
        from_high = jnp.logical_and(jnp.logical_not(up), place < length - 1)

        def take(slot):
            copy(slot % length, twin, slot).wait_recv()
            buffer[owner] = buffer[owner] + landed[slot]

        @pl.when(from_low)
        def _():
            take(owner)

        @pl.when(from_high)
        def _():
            take(jnp.where(mine, length, owner))

        @pl.when(jnp.logical_not(mine))
        def _():
            target, slot = ahead(owner)
            copy(owner, target, slot).start()

    def first_pass(j, carry):
        owner = owner_at(place, length, j)

        def product(block, narrow_row):
            own_b[owner, pl.ds(narrow_row, rows)] = jnp.dot(
                x_ref[block], y_ref[:, wide:total], preferred_element_type=jnp.float32
            )
            return jnp.dot(x_ref[block], y_ref[:, 0:wide], preferred_element_type=jnp.float32)

        pair_out[j] = product(owner * 2 + (1 - side), (1 - side) * rows)

        @pl.when(j == 0)
        def _():
            pair_copy(j).start()

        own[owner] = product(owner * 2 + side, side * rows)
        flow(owner, lineb_copy, own_b, line_in_b)
        return carry

    lax.fori_loop(0, length, first_pass, 0)

    def second_pass(j, carry):
        owner = owner_at(place, length, j)
        pair_copy(j).wait()

        @pl.when(j < length - 1)
        def _():
            pair_copy(j + 1).start()

        @pl.when(j == length - 1)
        def _():
            swap_copy().start()

        @pl.when(j == 0)
        def _():
            def push(k, inner):
                stat_copy(k).start()
                return inner

            lax.fori_loop(1, n, push, 0)

        own[owner] = own[owner] + pair_in[j]
        flow(owner, line_copy, own, line_in)
        return carry

    lax.fori_loop(0, length, second_pass, 0)
    out_ref[:, 0:wide] = own[place]
    swap_copy().wait()
    out_ref[:, wide:total] = own_b[place, pl.ds(side * rows, rows)] + swap_in[...]

    def settle(k, carry):
        stat_copy(k).wait()
        stats_ref[k] = st_in[k]
        return carry

    lax.fori_loop(1, n, settle, 0)
    stats_ref[0] = st_ref[me]

    def drain(owner, carry):
        @pl.when(owner != place)
        def _():
            lineb_copy(owner, twin, owner).wait_send()
            line_copy(owner, twin, owner).wait_send()

        return carry

    lax.fori_loop(0, length, drain, 0)


def reduce_blocks(blocks, columns, packed):
    n, rows, depth = blocks.shape
    total = columns.shape[1]
    narrow = max(128, total // 8 // 128 * 128)
    wide = total - narrow
    length = n // 2
    dma = pltpu.SemaphoreType.DMA
    f32 = jnp.float32
    vmem = pl.BlockSpec(memory_space=pltpu.VMEM)
    return pl.pallas_call(
        functools.partial(reduce_kernel, n),
        out_shape=(
            jax.ShapeDtypeStruct((rows, total), f32),
            jax.ShapeDtypeStruct(packed.shape, f32),
        ),
        in_specs=[vmem] * 3,
        out_specs=(vmem, vmem),
        scratch_shapes=[
            pltpu.VMEM((length, rows, wide), f32),
            pltpu.VMEM((length, rows, wide), f32),
            pltpu.VMEM((length, rows, wide), f32),
            pltpu.VMEM((length + 1, rows, wide), f32),
            pltpu.VMEM((length, 2 * rows, narrow), f32),
            pltpu.VMEM((length + 1, 2 * rows, narrow), f32),
            pltpu.VMEM((rows, narrow), f32),
            pltpu.VMEM(packed.shape, f32),
            dma((length,)), dma((length,)),
            dma((length,)), dma((length + 1,)),
            dma((length,)), dma((length + 1,)),
            dma((1,)), dma((1,)),
            dma((n,)), dma((n,)),
        ],
        name="reduce_blocks",
        compiler_params=pltpu.CompilerParams(
            collective_id=0, has_side_effects=True, vmem_limit_bytes=60 * 1024 * 1024
        ),
    )(blocks, columns, packed)


def per_device(view_first, view_second, valid_rows):
    local_rows = view_first.shape[0]
    feature_width = view_first.shape[1]
    column_width = view_second.shape[1]
    group_count = lax.axis_size("dp")
    block_rows = feature_width // group_count
    used_rows = valid_rows[0]
    used_float = used_rows.astype(jnp.float32)
    positions = lax.broadcasted_iota(jnp.int32, (local_rows, 1), 0)
    live_col = (positions < used_rows).astype(jnp.float32)
    live_row = jnp.transpose(live_col).astype(jnp.bfloat16)
    sum_first = jnp.dot(live_row, view_first, preferred_element_type=jnp.float32)[0]
    sum_second = jnp.dot(live_row, view_second, preferred_element_type=jnp.float32)[0]
    mean_first = sum_first / used_float
    mean_second = sum_second / used_float
    centered_first = ((view_first.astype(jnp.float32) - mean_first) * live_col).astype(jnp.bfloat16)
    centered_second = ((view_second.astype(jnp.float32) - mean_second) * live_col).astype(
        jnp.bfloat16
    )
    square_first = jnp.sum(jnp.square(centered_first.astype(jnp.float32)), axis=0)
    square_second = jnp.sum(jnp.square(centered_second.astype(jnp.float32)), axis=0)
    group_index = lax.axis_index("dp")
    row_start = group_index * block_rows
    shared = jnp.concatenate([sum_second, square_second, used_float[None]])
    packed = jnp.concatenate(
        [
            sum_first.reshape(group_count, block_rows),
            square_first.reshape(group_count, block_rows),
            jnp.broadcast_to(shared[None], (group_count, shared.shape[0])),
        ],
        axis=1,
    )
    filled = packed.shape[1]
    packed = jnp.pad(packed, ((0, 0), (0, -filled % 1024))).reshape(group_count, -1, 128)
    blocks = jnp.transpose(centered_first).reshape(group_count, block_rows, local_rows)
    moment, stats = reduce_blocks(blocks, centered_second, packed)
    stats = stats.reshape(group_count, -1)
    cuts = [block_rows, 2 * block_rows, 2 * block_rows + column_width, 2 * block_rows + 2 * column_width]
    sums_rows = stats[:, : cuts[0]]
    squares_rows = stats[:, cuts[0] : cuts[1]]
    sums_second = stats[:, cuts[1] : cuts[2]]
    squares_second = stats[:, cuts[2] : cuts[3]]
    counts_col = stats[:, cuts[3] : cuts[3] + 1]
    all_rows = jnp.sum(counts_col)
    glob_rows = jnp.sum(sums_rows, axis=0) / all_rows
    glob_second = jnp.sum(sums_second, axis=0) / all_rows
    owned_shift = sums_rows / counts_col - glob_rows[None, :]
    shifts_second = sums_second / counts_col - glob_second[None, :]
    spread_rows = jnp.sum(squares_rows + counts_col * jnp.square(owned_shift), axis=0)
    spread_second = jnp.sum(squares_second + counts_col * jnp.square(shifts_second), axis=0)
    weighted = owned_shift * counts_col
    moment = moment + lax.dot_general(
        weighted,
        shifts_second,
        (((0,), (0,)), ((), ())),
        precision=lax.Precision.HIGHEST,
        preferred_element_type=jnp.float32,
    )
    scale_rows = jnp.sqrt(spread_rows / all_rows + epsilon)
    scale_cols = jnp.sqrt(spread_second / all_rows + epsilon)
    correlation = moment / (all_rows * scale_rows[:, None] * scale_cols[None, :])
    col_start = lax.axis_index("col") * column_width
    global_rows = row_start + lax.broadcasted_iota(jnp.int32, (block_rows, 1), 0)
    global_cols = col_start + lax.broadcasted_iota(jnp.int32, (1, column_width), 1)
    diagonal = global_rows == global_cols
    terms = jnp.where(diagonal, jnp.square(1.0 - correlation), off_weight * jnp.square(correlation))
    partial_loss = jnp.sum(terms)
    loss = lax.psum(partial_loss, ("dp", "col")) / feature_width
    return (correlation, loss)


def solution(mesh):
    return jax.shard_map(
        per_device,
        mesh=mesh,
        in_specs=(P("dp", None), P("dp", "col"), P("dp")),
        out_specs=(P("dp", "col"), P()),
        check_vma=False,
    )
```

```python
import functools
import jax
import jax.numpy as jnp
from jax import lax
from jax.experimental import pallas as pl
from jax.experimental.pallas import tpu as pltpu
from jax.sharding import PartitionSpec as P

epsilon = 1e-05
off_weight = 0.0051
MESH = pl.DeviceIdType.MESH


def owner_at(place, length, step):
    low = jnp.minimum(place, length - 1 - place)
    high = length - 1 - low
    single = high - low
    rest = step - single
    upward = jnp.where(step < single, place == low, rest % 2 == 0)
    reach = jnp.where(step < single, high - step, low - rest // 2)
    return jnp.where(upward, place + reach, place - reach)


def reduce_kernel(
    n, x_ref, y_ref, sum_ref, tail_ref, out_ref, first_ref, second_ref,
    terms, pair_in, line_in, own_b, line_in_b, swap_in, sf, sy, sf_in, sy_in,
    pair_ss, pair_rs, line_ss, line_rs, lineb_ss, lineb_rs, swap_ss, swap_rs,
    sf_ss, sf_rs, sy_ss, sy_rs,
):
    me = lax.axis_index("dp")
    length = n // 2
    place, side = me // 2, me % 2
    twin = place * 2 + (1 - side)
    rows = terms.shape[2]
    wide = terms.shape[3]
    total = y_ref.shape[1]

    barrier = pltpu.get_barrier_semaphore()

    def greet(k, carry):
        pl.semaphore_signal(barrier, inc=1, device_id={"dp": (me + k) % n}, device_id_type=MESH)
        return carry

    lax.fori_loop(1, n, greet, 0)
    pl.semaphore_wait(barrier, n - 1)

    def remote(src, dst, ss, rs, target):
        return pltpu.make_async_remote_copy(
            src_ref=src, dst_ref=dst, send_sem=ss, recv_sem=rs,
            device_id={"dp": target}, device_id_type=MESH,
        )

    def first_copy(k):
        peer = (me + k) % n
        return remote(sf.at[peer // 2], sf_in.at[k], sf_ss.at[k], sf_rs.at[k], peer)

    def second_copy(k):
        return remote(sy, sy_in.at[k], sy_ss.at[k], sy_rs.at[k], (me + k) % n)

    def pair_copy(j):
        source = terms.at[owner_at(place, length, j), 1 - side]
        return remote(source, pair_in.at[j], pair_ss.at[j], pair_rs.at[j], twin)

    def ahead(owner):
        up = owner > place
        nearer = jnp.where(up, place + 1, place - 1)
        slot = jnp.where(jnp.logical_and(owner == nearer, jnp.logical_not(up)), length, owner)
        return nearer * 2 + side, slot

    def line_copy(owner, target, slot):
        return remote(terms.at[owner, side], line_in.at[slot], line_ss.at[owner], line_rs.at[slot], target)

    def lineb_copy(owner, target, slot):
        return remote(own_b.at[owner], line_in_b.at[slot], lineb_ss.at[owner], lineb_rs.at[slot], target)

    def swap_copy():
        return remote(
            own_b.at[place, pl.ds((1 - side) * rows, rows)], swap_in, swap_ss.at[0], swap_rs.at[0], twin
        )

    def flow(owner, copy, at, buffer, landed):
        up = owner > place
        mine = owner == place
        from_low = jnp.logical_and(jnp.logical_or(up, mine), place > 0)
        from_high = jnp.logical_and(jnp.logical_not(up), place < length - 1)

        def take(slot):
            copy(slot % length, twin, slot).wait_recv()
            buffer[at] = buffer[at] + landed[slot]

        @pl.when(from_low)
        def _():
            take(owner)

        @pl.when(from_high)
        def _():
            take(jnp.where(mine, length, owner))

        @pl.when(jnp.logical_not(mine))
        def _():
            target, slot = ahead(owner)
            copy(owner, target, slot).start()

    def first_pass(j, carry):
        owner = owner_at(place, length, j)

        start = pl.multiple_of(owner * (2 * rows), 2 * rows)
        pair = x_ref[:, pl.ds(start, 2 * rows)]

        def product(low, high):
            return lax.dot_general(
                pair, y_ref[:, low:high], (((0,), (0,)), ((), ())),
                preferred_element_type=jnp.float32,
            )

        both = product(0, wide)
        terms[owner, 0] = both[:rows]
        terms[owner, 1] = both[rows:]

        @pl.when(j == 0)
        def _():
            pair_copy(j).start()

        own_b[owner] = product(wide, total)
        squares = jnp.sum(jnp.square(pair.astype(jnp.float32)), axis=0, keepdims=True)
        line = lax.broadcasted_iota(jnp.int32, (8, 2 * rows), 0)
        sf[owner] = jnp.where(line == 0, sum_ref[owner], squares)
        flow(owner, lineb_copy, owner, own_b, line_in_b)
        return carry

    lax.fori_loop(0, length, first_pass, 0)
    squares = jnp.sum(jnp.square(y_ref[...].astype(jnp.float32)), axis=0, keepdims=True)
    line = lax.broadcasted_iota(jnp.int32, (8, total), 0)
    sy[...] = jnp.where(line == 0, tail_ref[0:1], jnp.where(line == 1, squares, tail_ref[1:2]))

    def second_pass(j, carry):
        owner = owner_at(place, length, j)
        pair_copy(j).wait()

        @pl.when(j < length - 1)
        def _():
            pair_copy(j + 1).start()

        @pl.when(j == length - 1)
        def _():
            swap_copy().start()

        @pl.when(j == 0)
        def _():
            def push(k, inner):
                first_copy(k).start()
                second_copy(k).start()
                return inner

            lax.fori_loop(1, n, push, 0)

        terms[owner, side] = terms[owner, side] + pair_in[j]
        flow(owner, line_copy, (owner, side), terms, line_in)
        return carry

    lax.fori_loop(0, length, second_pass, 0)
    out_ref[:, 0:wide] = terms[place, side]
    swap_copy().wait()
    out_ref[:, wide:total] = own_b[place, pl.ds(side * rows, rows)] + swap_in[...]

    def settle(k, carry):
        first_copy(k).wait()
        second_copy(k).wait()
        first_ref[k] = sf_in[k]
        second_ref[k] = sy_in[k]
        return carry

    lax.fori_loop(1, n, settle, 0)
    first_ref[0] = sf[place]
    second_ref[0] = sy[...]

    def drain(owner, carry):
        @pl.when(owner != place)
        def _():
            lineb_copy(owner, twin, owner).wait_send()
            line_copy(owner, twin, owner).wait_send()

        return carry

    lax.fori_loop(0, length, drain, 0)


def reduce_blocks(n, first, columns, sums, tail):
    rows = first.shape[1] // n
    total = columns.shape[1]
    narrow = max(128, total // 8 // 128 * 128)
    wide = total - narrow
    length = n // 2
    dma = pltpu.SemaphoreType.DMA
    f32 = jnp.float32
    vmem = pl.BlockSpec(memory_space=pltpu.VMEM)
    return pl.pallas_call(
        functools.partial(reduce_kernel, n),
        out_shape=(
            jax.ShapeDtypeStruct((rows, total), f32),
            jax.ShapeDtypeStruct((n, 8, 2 * rows), f32),
            jax.ShapeDtypeStruct((n, 8, total), f32),
        ),
        in_specs=[vmem] * 4,
        out_specs=(vmem, vmem, vmem),
        scratch_shapes=[
            pltpu.VMEM((length, 2, rows, wide), f32),
            pltpu.VMEM((length, rows, wide), f32),
            pltpu.VMEM((length + 1, rows, wide), f32),
            pltpu.VMEM((length, 2 * rows, narrow), f32),
            pltpu.VMEM((length + 1, 2 * rows, narrow), f32),
            pltpu.VMEM((rows, narrow), f32),
            pltpu.VMEM((length, 8, 2 * rows), f32),
            pltpu.VMEM((8, total), f32),
            pltpu.VMEM((n, 8, 2 * rows), f32),
            pltpu.VMEM((n, 8, total), f32),
            dma((length,)), dma((length,)),
            dma((length,)), dma((length + 1,)),
            dma((length,)), dma((length + 1,)),
            dma((1,)), dma((1,)),
            dma((n,)), dma((n,)), dma((n,)), dma((n,)),
        ],
        name="reduce_blocks",
        compiler_params=pltpu.CompilerParams(
            collective_id=0, has_side_effects=True, vmem_limit_bytes=60 * 1024 * 1024
        ),
    )(first, columns, sums, tail)


def total_kernel(n, m, part_ref, out_ref, held, line, across, ss, rs, ss2, rs2):
    me, col = lax.axis_index("dp"), lax.axis_index("col")
    barrier = pltpu.get_barrier_semaphore()

    def each(count, body):
        def step(k, carry):
            body(k)
            return carry

        lax.fori_loop(1, count, step, 0)

    def greet(axis, index, count):
        return lambda k: pl.semaphore_signal(
            barrier, inc=1, device_id={axis: (index + k) % count}, device_id_type=MESH
        )

    each(n, greet("dp", me, n))
    each(m, greet("col", col, m))
    pl.semaphore_wait(barrier, n + m - 2)

    def dp_copy(k):
        return pltpu.make_async_remote_copy(
            src_ref=part_ref, dst_ref=line.at[me], send_sem=ss.at[k], recv_sem=rs.at[k],
            device_id={"dp": (me + k) % n}, device_id_type=MESH,
        )

    def col_copy(k):
        return pltpu.make_async_remote_copy(
            src_ref=held, dst_ref=across.at[col], send_sem=ss2.at[k], recv_sem=rs2.at[k],
            device_id={"col": (col + k) % m}, device_id_type=MESH,
        )

    each(n, lambda k: dp_copy(k).start())
    line[me] = part_ref[...]
    each(n, lambda k: dp_copy(k).wait())
    held[...] = jnp.sum(line[...], axis=0)
    each(m, lambda k: col_copy(k).start())
    across[col] = held[...]
    each(m, lambda k: col_copy(k).wait())
    out_ref[...] = jnp.sum(across[...], axis=0)


def add_everywhere(n, m, value):
    f32 = jnp.float32
    vmem = pl.BlockSpec(memory_space=pltpu.VMEM)
    dma = pltpu.SemaphoreType.DMA
    tile = (8, 128)
    return pl.pallas_call(
        functools.partial(total_kernel, n, m),
        out_shape=jax.ShapeDtypeStruct(tile, f32),
        in_specs=[vmem],
        out_specs=vmem,
        scratch_shapes=[
            pltpu.VMEM(tile, f32),
            pltpu.VMEM((n,) + tile, f32),
            pltpu.VMEM((m,) + tile, f32),
            dma((n,)), dma((n,)), dma((m,)), dma((m,)),
        ],
        name="add_everywhere",
        compiler_params=pltpu.CompilerParams(collective_id=1, has_side_effects=True),
    )(jnp.broadcast_to(value, tile))[0, 0]


def per_device(view_first, view_second, valid_rows):
    local_rows = view_first.shape[0]
    feature_width = view_first.shape[1]
    column_width = view_second.shape[1]
    group_count = lax.axis_size("dp")
    block_rows = feature_width // group_count
    used_rows = valid_rows[0]
    used_float = used_rows.astype(jnp.float32)
    positions = lax.broadcasted_iota(jnp.int32, (local_rows, 1), 0)
    live_col = (positions < used_rows).astype(jnp.float32)
    live_row = jnp.transpose(live_col).astype(jnp.bfloat16)
    sum_first = jnp.dot(live_row, view_first, preferred_element_type=jnp.float32)[0]
    sum_second = jnp.dot(live_row, view_second, preferred_element_type=jnp.float32)[0]
    mean_first = sum_first / used_float
    mean_second = sum_second / used_float
    centered_first = ((view_first.astype(jnp.float32) - mean_first) * live_col).astype(jnp.bfloat16)
    centered_second = ((view_second.astype(jnp.float32) - mean_second) * live_col).astype(
        jnp.bfloat16
    )
    group_index = lax.axis_index("dp")
    row_start = group_index * block_rows
    tail = jnp.stack([sum_second, jnp.broadcast_to(used_float, sum_second.shape)])
    sums = sum_first.reshape(group_count // 2, 1, 2 * block_rows)
    moment, stats_first, stats_second = reduce_blocks(
        group_count, centered_first, centered_second, sums, tail
    )
    stats_first = lax.dynamic_slice_in_dim(
        stats_first[:, :2], group_index % 2 * block_rows, block_rows, 2
    )
    sums_rows, squares_rows = stats_first[:, 0], stats_first[:, 1]
    sums_second, squares_second = stats_second[:, 0], stats_second[:, 1]
    counts_col = stats_second[:, 2, :1]
    all_rows = jnp.sum(counts_col)
    glob_rows = jnp.sum(sums_rows, axis=0) / all_rows
    glob_second = jnp.sum(sums_second, axis=0) / all_rows
    owned_shift = sums_rows / counts_col - glob_rows[None, :]
    shifts_second = sums_second / counts_col - glob_second[None, :]
    spread_rows = jnp.sum(squares_rows + counts_col * jnp.square(owned_shift), axis=0)
    spread_second = jnp.sum(squares_second + counts_col * jnp.square(shifts_second), axis=0)
    weighted = owned_shift * counts_col
    moment = moment + lax.dot_general(
        weighted,
        shifts_second,
        (((0,), (0,)), ((), ())),
        precision=lax.Precision.HIGHEST,
        preferred_element_type=jnp.float32,
    )
    scale_rows = jnp.sqrt(spread_rows / all_rows + epsilon)
    scale_cols = jnp.sqrt(spread_second / all_rows + epsilon)
    correlation = moment / (all_rows * scale_rows[:, None] * scale_cols[None, :])
    col_start = lax.axis_index("col") * column_width
    global_rows = row_start + lax.broadcasted_iota(jnp.int32, (block_rows, 1), 0)
    global_cols = col_start + lax.broadcasted_iota(jnp.int32, (1, column_width), 1)
    diagonal = global_rows == global_cols
    terms = jnp.where(diagonal, jnp.square(1.0 - correlation), off_weight * jnp.square(correlation))
    partial_loss = jnp.sum(terms)
    loss = add_everywhere(group_count, lax.axis_size("col"), partial_loss) / feature_width
    return (correlation, loss)


def solution(mesh):
    return jax.shard_map(
        per_device,
        mesh=mesh,
        in_specs=(P("dp", None), P("dp", "col"), P("dp")),
        out_specs=(P("dp", "col"), P()),
        check_vma=False,
    )
```
